32 devices in a mesh: rows: 8 (over y, x, core), grp: 4 (over z).
Axes of the slice: x: 2, y: 2, z: 4, core: 2. Of those that a mesh axis runs over, the one named last changes fastest.
Arguments:
- pivot_columns: bfloat16 [32, 10240, 256], P('rows', 'grp'), may hold values from -6 to 6
- previous: bfloat16 [32, 10240, 512], P('rows', 'grp'), may hold values from -0.59765625 to 0.59765625
- pivots: int32 [256], replicated, may hold values from 0 to 327679, as said below
- pivot_inverse: bfloat16 [256, 256], replicated, may hold values from -0.4 to 1.5
- orbitals: bfloat16 [10240, 1024], P('grp'), may hold values from -0.0625 to 0.0625
- slab_orbitals: bfloat16 [32, 1024], replicated, may hold values from -1 to 1
Outputs:
- new_vectors: bfloat16 [32, 10240, 256], P('rows', 'grp')
- mo_block: bfloat16 [256, 1024, 1024], P('rows', None, 'grp')
The draws below stay inside these ranges and needn't reach their ends.
Inputs may be any that keep to these rules, and one draw needn't show every extreme that they name: `pivots`: distinct entries.
All inputs are finite; a program needn't handle non-finite values.
Results may differ from the reference program's by a relative error of at most 0.0038.
The reference program's roundings to bfloat16 on the way (of `pivot_rows`, `residual_columns`, `upper` and `half`) count: a program that leaves them out, or rounds other values in their place, can miss the bound.
Values may be sent and summed in bfloat16 or wider, within the bound.
A program may use at most 128 MiB of HBM per device.

```python
import jax
import jax.numpy as jnp

NBAS = 10240
NOCC = 1024
K_PREV = 512
NP = 256
MU = 32


def draw_pivots(key, part):
    chosen = jax.random.permutation(key, MU * NBAS)[:NP]
    return chosen.astype(jnp.int32)


def draw_pivot_inverse(key, part):
    first, second = jax.random.split(jax.random.fold_in(key, 17))
    spread = jax.random.normal(first, (NP, NP), jnp.float32) * NP ** (-0.5)
    spread = jnp.clip(spread, -0.39, 0.39)
    diagonal = jax.random.uniform(second, (NP,), jnp.float32, 0.5, 1.5)
    eye_mask = jnp.arange(NP)[:, None] == jnp.arange(NP)[None, :]
    return jnp.where(eye_mask, diagonal[None, :], spread).astype(jnp.bfloat16)


def shard_levels(key, dims, cuts, low, largest):
    loudness = 1.0
    for position, blocks in cuts:
        heights = jax.random.uniform(jax.random.fold_in(jax.random.fold_in(key, 6), position), (blocks,), jnp.float32, low / len(cuts), largest / len(cuts))
        loudness = loudness * jnp.repeat(jnp.exp(heights), dims[position] // blocks).reshape((-1,) + (1,) * (len(dims) - 1 - position))
    return loudness


def scatter_about(rng, dims, deviation, reach, shards=(), dtype=jnp.bfloat16):
    entries = deviation * jax.random.normal(rng, dims, jnp.float32)
    if shards:
        entries = entries * shard_levels(rng, dims, shards, -0.22, 0.18)
    return jnp.clip(entries, -reach, reach).astype(dtype)


def setup_inputs(seed: int = 0) -> dict:
    arg_keys = jax.random.split(jax.random.key(seed), 7)
    return {
        "pivot_columns": scatter_about(arg_keys[0], (MU, NBAS, NP), 1.0, 6.0, ((0, 8), (1, 4))),
        "previous": scatter_about(arg_keys[1], (MU, NBAS, K_PREV), 0.1, 0.59765625, ((0, 8), (1, 4))),
        "pivots": draw_pivots(jax.random.fold_in(arg_keys[6], 71), 0),
        "pivot_inverse": draw_pivot_inverse(jax.random.fold_in(arg_keys[6], 71), 0),
        "orbitals": scatter_about(arg_keys[4], (NBAS, NOCC), NBAS ** -0.5, 0.0625, ((0, 4),)),
        "slab_orbitals": scatter_about(arg_keys[5], (MU, NOCC), MU ** -0.5, 1.0),
    }


def reference(pivot_columns, previous, pivots, pivot_inverse, orbitals, slab_orbitals):
    prev_count = previous.shape[2]
    flat_prev = previous.reshape(MU * NBAS, prev_count)
    pivot_rows = jnp.take(flat_prev, pivots.astype(jnp.int32), axis=0)
    correction = jnp.dot(flat_prev, pivot_rows.T, preferred_element_type=jnp.float32)
    flat_columns = pivot_columns.reshape(MU * NBAS, NP)
    residual_columns = (flat_columns.astype(jnp.float32) - correction).astype(jnp.bfloat16)
    upper = jnp.triu(pivot_inverse)
    new_flat = jnp.dot(residual_columns, upper, preferred_element_type=jnp.float32).astype(jnp.bfloat16)
    new_vectors = new_flat.reshape(MU, NBAS, NP)
    by_second = jnp.transpose(new_vectors, (1, 0, 2)).reshape(NBAS, MU * NP)
    half = jnp.dot(orbitals.T, by_second, preferred_element_type=jnp.float32).astype(jnp.bfloat16)
    half = half.reshape(NOCC, MU, NP)
    by_first = jnp.transpose(half, (1, 0, 2)).reshape(MU, NOCC * NP)
    full = jnp.dot(slab_orbitals.T, by_first, preferred_element_type=jnp.float32).astype(jnp.bfloat16)
    mo_block = jnp.transpose(full.reshape(NOCC, NOCC, NP), (2, 0, 1))
    return new_vectors, mo_block
```

```python
import functools

import jax
import jax.numpy as jnp
from jax import lax
from jax.experimental import pallas as pl
from jax.experimental.pallas import tpu as pltpu
from jax.sharding import PartitionSpec as P

F32 = jnp.float32
BF16 = jnp.bfloat16
MESH = pl.DeviceIdType.MESH


def exchange_kernel(R, G, x_ref, o_ref, buf_a, buf_b, buf_c, send_a, recv_a, send_b, recv_b, send_c, recv_c):
    r = lax.axis_index("rows")
    g = lax.axis_index("grp")
    row_peers = [(d, lax.rem(r + d, R)) for d in range(1, R)]
    grp_peers = [(d, lax.rem(g + d, G)) for d in range(1, G)]
    barrier = pltpu.get_barrier_semaphore()
    for _, peer in row_peers:
        pl.semaphore_signal(barrier, inc=1, device_id={"rows": peer, "grp": g}, device_id_type=MESH)
    for _, peer in grp_peers:
        pl.semaphore_signal(barrier, inc=1, device_id={"rows": r, "grp": peer}, device_id_type=MESH)
    pl.semaphore_wait(barrier, R - 1 + G - 1)

    def remote(src, dst, send, recv, device):
        return pltpu.make_async_remote_copy(
            src_ref=src, dst_ref=dst, send_sem=send, recv_sem=recv, device_id={"rows": device[0], "grp": device[1]}, device_id_type=MESH
        )

    first = [remote(x_ref.at[p], buf_a.at[d], send_a.at[d], recv_a.at[d], (p, g)) for d, p in row_peers]
    for copy in first:
        copy.start()
    total = x_ref[r].astype(F32)
    for (d, _), copy in zip(row_peers, first):
        copy.wait_recv()
        total = total + buf_a[d].astype(F32)
    buf_b[0] = total.astype(BF16)
    second = [remote(buf_b.at[0], buf_b.at[d], send_b.at[d], recv_b.at[d], (r, p)) for d, p in grp_peers]
    for copy in second:
        copy.start()
    for (d, _), copy in zip(grp_peers, second):
        copy.wait_recv()
        total = total + buf_b[d].astype(F32)
    buf_c[r] = total.astype(BF16)
    third = [remote(buf_c.at[r], buf_c.at[r], send_c.at[d], recv_c.at[d], (p, g)) for d, p in row_peers]
    for copy in third:
        copy.start()
    for copy in third:
        copy.wait_recv()
    for copy in first + second + third:
        copy.wait_send()
    o_ref[...] = buf_c[...]


def exchange(x, R, G):
    vmem = pl.BlockSpec(memory_space=pltpu.VMEM)
    _, c, k = x.shape
    dma = pltpu.SemaphoreType.DMA
    return pl.pallas_call(
        functools.partial(exchange_kernel, R, G),
        out_shape=jax.ShapeDtypeStruct(x.shape, BF16),
        in_specs=[vmem],
        out_specs=vmem,
        scratch_shapes=[
            pltpu.VMEM((R, c, k), BF16),
            pltpu.VMEM((G, c, k), BF16),
            pltpu.VMEM((R, c, k), BF16),
            dma((R,)), dma((R,)), dma((G,)), dma((G,)), dma((R,)), dma((R,)),
        ],
        compiler_params=pltpu.CompilerParams(collective_id=0, has_side_effects=True),
        name="pivot_exchange",
    )(x)


def vectors_kernel(pc_ref, prev_ref, rows_ref, inv_ref, out_ref):
    correction = lax.dot_general(
        prev_ref[...], rows_ref[...], (((1,), (1,)), ((), ())), preferred_element_type=F32
    )
    residual = (pc_ref[...].astype(F32) - correction).astype(BF16)
    shape = inv_ref.shape
    keep = lax.broadcasted_iota(jnp.int32, shape, 0) <= lax.broadcasted_iota(jnp.int32, shape, 1)
    upper = jnp.where(keep, inv_ref[...].astype(F32), 0.0).astype(BF16)
    out_ref[...] = jnp.dot(residual, upper, preferred_element_type=F32).astype(BF16)


def vectors(columns, prev, rows, inverse):
    m, p = columns.shape
    k = prev.shape[1]
    tile = 1024
    while m % tile:
        tile //= 2
    return pl.pallas_call(
        vectors_kernel,
        grid=(m // tile,),
        out_shape=jax.ShapeDtypeStruct((m, p), BF16),
        in_specs=[
            pl.BlockSpec((tile, p), lambda i: (i, 0)),
            pl.BlockSpec((tile, k), lambda i: (i, 0)),
            pl.BlockSpec((p, k), lambda i: (0, 0)),
            pl.BlockSpec((p, p), lambda i: (0, 0)),
        ],
        out_specs=pl.BlockSpec((tile, p), lambda i: (i, 0)),
        name="new_vectors",
    )(columns, prev, rows, inverse)


def half_kernel(R, G, new_hbm, orb_hbm, out_hbm, new_v, orb_v, turned, send, in_sem, own_sem, send_sem, recv_sem):
    r = lax.axis_index("rows")
    g = lax.axis_index("grp")
    N = R * G
    mu_dev, nu, p = new_v.shape
    _, _, _, pl_dev, j_dev = send.shape

    def load(mu):
        return pltpu.make_async_copy(new_hbm.at[mu], new_v.at[mu], in_sem.at[mu])

    load_orb = pltpu.make_async_copy(orb_hbm, orb_v, in_sem.at[mu_dev])
    load(0).start()
    load_orb.start()
    for mu in range(1, mu_dev):
        load(mu).start()

    barrier = pltpu.get_barrier_semaphore()
    me = r * G + g

    @pl.loop(1, N)
    def _(d):
        peer = lax.rem(me + d, N)
        pl.semaphore_signal(
            barrier, inc=1, device_id={"rows": peer // G, "grp": lax.rem(peer, G)}, device_id_type=MESH
        )

    chunk = 256
    shape = (p, p)
    eye = jnp.where(
        lax.broadcasted_iota(jnp.int32, shape, 0) == lax.broadcasted_iota(jnp.int32, shape, 1), 1.0, 0.0
    ).astype(BF16)

    def turn(mu):
        @pl.loop(0, nu // chunk)
        def _(i):
            at = pl.ds(pl.multiple_of(i * chunk, chunk), chunk)
            turned[:, at] = lax.dot_general(
                eye, new_v[mu, at, :], (((1,), (1,)), ((), ())), preferred_element_type=F32
            ).astype(BF16)

    pl.semaphore_wait(barrier, N - 1)
    load_orb.wait()

    @pl.loop(0, mu_dev)
    def _(mu):
        load(mu).wait()
        turn(mu)
        slot = (g * R + r) * mu_dev + mu

        @pl.loop(0, G)
        def _(d):
            to = lax.rem(g + 1 + d, G)
            cols = pl.ds(pl.multiple_of(to * j_dev, j_dev), j_dev)
            block = jnp.dot(turned[...], orb_v[:, cols], preferred_element_type=F32)
            for k in range(R):
                send[mu, to, k] = block[k * pl_dev : (k + 1) * pl_dev].astype(BF16)

            for k in range(R):
                peer = lax.rem(r + k, R)
                src = send.at[mu, to, peer]
                dst = out_hbm.at[slot]

                def away():
                    pltpu.make_async_remote_copy(
                        src_ref=src, dst_ref=dst, send_sem=send_sem, recv_sem=recv_sem,
                        device_id={"rows": peer, "grp": to}, device_id_type=MESH,
                    ).start()

                if k:
                    away()
                else:
                    pl.when(to != g)(away)

                    @pl.when(to == g)
                    def _():
                        pltpu.make_async_copy(src, dst, own_sem).start()

    others = out_hbm.at[pl.ds(0, (N - 1) * mu_dev)]
    own = out_hbm.at[pl.ds(0, mu_dev)]
    pltpu.make_async_copy(own, own, own_sem).wait()
    pltpu.make_async_copy(others, others, send_sem).wait()
    pltpu.make_async_copy(others, others, recv_sem).wait()


def half_partials(new, orbitals, R, G):
    mu_dev, nu, p = new.shape
    nj = orbitals.shape[1]
    hbm = pl.BlockSpec(memory_space=pl.ANY)
    dma = pltpu.SemaphoreType.DMA
    return pl.pallas_call(
        functools.partial(half_kernel, R, G),
        out_shape=jax.ShapeDtypeStruct((R * G * mu_dev, p // R, nj // G), BF16),
        in_specs=[hbm, hbm],
        out_specs=hbm,
        scratch_shapes=[
            pltpu.VMEM((mu_dev, nu, p), BF16),
            pltpu.VMEM((nu, nj), BF16),
            pltpu.VMEM((p, nu), BF16),
            pltpu.VMEM((mu_dev, G, R, p // R, nj // G), BF16),
            dma((mu_dev + 1,)), dma(()), dma(()), dma(()),
        ],
        compiler_params=pltpu.CompilerParams(collective_id=1, has_side_effects=True),
        name="half_exchange",
    )(new, orbitals)


def block_kernel(part_ref, slab_ref, out_ref, half_ref, sorted_ref, slab_t_ref):
    groups, rows, _ = part_ref.shape
    mus = slab_ref.shape[0]
    block = out_ref.shape[0]
    vecs = rows // mus
    step = pl.program_id(0)

    @pl.when(step == 0)
    def _():
        slab_t_ref[...] = slab_ref[...].astype(F32).T.astype(BF16)
        piece = 128

        @pl.loop(0, rows // piece)
        def _(i):
            at = pl.ds(pl.multiple_of(i * piece, piece), piece)
            total = part_ref[0, at, :].astype(F32)
            for k in range(1, groups):
                total = total + part_ref[k, at, :].astype(F32)
            half_ref[at, :] = total.astype(BF16)

        shift = mus.bit_length() - 1

        @pl.loop(0, rows // piece)
        def _(i):
            at = pl.ds(pl.multiple_of(i * piece, piece), piece)
            row = lax.broadcasted_iota(jnp.int32, (piece, rows), 0) + i * piece
            col = lax.broadcasted_iota(jnp.int32, (piece, rows), 1)
            source = (row & (mus - 1)) * vecs + lax.shift_right_logical(row, shift)
            pick = jnp.where(source == col, 1.0, 0.0).astype(BF16)
            sorted_ref[at, :] = jnp.dot(pick, half_ref[...], preferred_element_type=F32).astype(BF16)

    for q in range(block):
        at = pl.ds(pl.multiple_of((step * block + q) * mus, mus), mus)
        out_ref[q] = jnp.dot(slab_t_ref[...], sorted_ref[at, :], preferred_element_type=F32).astype(BF16)


def orbital_block(parts, slab):
    groups, rows, j = parts.shape
    mus, i = slab.shape
    assert mus & (mus - 1) == 0
    vecs = rows // mus
    block = 4 if vecs % 4 == 0 else 1
    return pl.pallas_call(
        block_kernel,
        grid=(vecs // block,),
        out_shape=jax.ShapeDtypeStruct((vecs, i, j), BF16),
        in_specs=[
            pl.BlockSpec((groups, rows, j), lambda s: (0, 0, 0)),
            pl.BlockSpec((mus, i), lambda s: (0, 0)),
        ],
        out_specs=pl.BlockSpec((block, i, j), lambda s: (s, 0, 0)),
        scratch_shapes=[
            pltpu.VMEM((rows, j), BF16),
            pltpu.VMEM((rows, j), BF16),
            pltpu.VMEM((i, mus), BF16),
        ],
        name="orbital_block",
    )(parts, slab)


def per_device(R, G, pivot_columns, previous, pivots, pivot_inverse, orbitals, slab_orbitals):
    mu_dev, nu_dev, prev_count = previous.shape
    count = pivot_columns.shape[2]
    nbas = nu_dev * G
    row_index = lax.axis_index("rows")
    grp_index = lax.axis_index("grp")
    first_local = pivots // nbas - row_index * mu_dev
    second_local = pivots % nbas - grp_index * nu_dev
    owned = (
        (first_local >= 0) & (first_local < mu_dev) & (second_local >= 0) & (second_local < nu_dev)
    )
    local_row = jnp.where(owned, first_local * nu_dev + second_local, 0)
    flat_prev = previous.reshape(mu_dev * nu_dev, prev_count)
    picked = jnp.where(
        owned[:, None], flat_prev.at[local_row].get(mode="promise_in_bounds"), jnp.zeros((), BF16)
    )
    pivot_rows = exchange(picked.reshape(R, count // R, prev_count), R, G).reshape(count, prev_count)
    new_flat = vectors(pivot_columns.reshape(-1, count), flat_prev, pivot_rows, pivot_inverse)
    new_vectors = new_flat.reshape(mu_dev, nu_dev, count)
    parts = half_partials(new_vectors, orbitals, R, G)
    parts = parts.reshape(G, R * mu_dev * (count // R), orbitals.shape[1] // G)
    return new_vectors, orbital_block(parts, slab_orbitals)


def solution(mesh):
    R, G = mesh.shape["rows"], mesh.shape["grp"]
    in_specs = (P("rows", "grp", None), P("rows", "grp", None), P(), P(), P("grp", None), P())
    out_specs = (P("rows", "grp", None), P("rows", None, "grp"))
    return jax.shard_map(
        functools.partial(per_device, R, G), mesh=mesh, in_specs=in_specs, out_specs=out_specs,
        check_vma=False,
    )
```

```python
import functools

import jax
import jax.numpy as jnp
from jax import lax
from jax.experimental import pallas as pl
from jax.experimental.pallas import tpu as pltpu
from jax.sharding import PartitionSpec as P

F32 = jnp.float32
BF16 = jnp.bfloat16
MESH = pl.DeviceIdType.MESH


def relayed(G):
    return G >= 4


def fused_kernel(
    R, G, x_ref, pc_hbm, prev_hbm, inv_ref, orb_hbm, out_hbm, new_hbm,
    buf_a, buf_b, buf_c, rows_wide, rows_v, upper_v, new_v, prev_v, orb_v, turned, block_v, send, relay,
    send_a, recv_a, send_b, recv_b, send_c, recv_c, in_sem, new_sem, own_sem, send_sem, recv_sem, relay_sem,
):
    r = lax.axis_index("rows")
    g = lax.axis_index("grp")
    N = R * G
    me = r * G + g
    mu_dev, nu, p = new_v.shape
    _, _, _, pl_dev, j_dev = send.shape
    c = buf_c.shape[1]

    def load(mu):
        return (
            pltpu.make_async_copy(prev_hbm.at[mu], prev_v.at[mu], in_sem.at[2 * mu]),
            pltpu.make_async_copy(pc_hbm.at[mu], new_v.at[mu], in_sem.at[2 * mu + 1]),
        )

    load_orb = pltpu.make_async_copy(orb_hbm, orb_v, in_sem.at[2 * mu_dev])
    for mu in range(mu_dev):
        for copy in load(mu):
            copy.start()
        if mu == 0:
            load_orb.start()

    barrier = pltpu.get_barrier_semaphore()

    @pl.loop(1, N)
    def _(d):
        peer = lax.rem(me + d, N)
        pl.semaphore_signal(
            barrier, inc=1, device_id={"rows": peer // G, "grp": lax.rem(peer, G)}, device_id_type=MESH
        )

    shape = (p, p)
    low = lax.broadcasted_iota(jnp.int32, shape, 0)
    high = lax.broadcasted_iota(jnp.int32, shape, 1)
    upper_v[...] = jnp.where(low <= high, inv_ref[...].astype(F32), 0.0).astype(BF16)
    pl.semaphore_wait(barrier, N - 1)

    def remote(src, dst, send, recv, row, grp):
        return pltpu.make_async_remote_copy(
            src_ref=src, dst_ref=dst, send_sem=send, recv_sem=recv,
            device_id={"rows": row, "grp": grp}, device_id_type=MESH,
        )

    row_peers = [(d, lax.rem(r + d, R)) for d in range(1, R)]
    grp_peers = [(d, lax.rem(g + d, G)) for d in range(1, G)]
    first = [remote(x_ref.at[q], buf_a.at[d], send_a.at[d], recv_a.at[d], q, g) for d, q in row_peers]
    for copy in first:
        copy.start()
    total = x_ref[r].astype(F32)
    for (d, _), copy in zip(row_peers, first):
        copy.wait_recv()
        total = total + buf_a[d].astype(F32)
    buf_b[0] = total.astype(BF16)
    second = [remote(buf_b.at[0], buf_b.at[d], send_b.at[d], recv_b.at[d], r, q) for d, q in grp_peers]
    for copy in second:
        copy.start()
    for (d, _), copy in zip(grp_peers, second):
        copy.wait_recv()
        total = total + buf_b[d].astype(F32)
    buf_c[r] = total.astype(BF16)
    third = [remote(buf_c.at[r], buf_c.at[r], send_c.at[d], recv_c.at[d], q, g) for d, q in row_peers]
    for copy in third:
        copy.start()
    for copy in third:
        copy.wait_recv()
    for copy in first + second + third:
        copy.wait_send()
    for k in range(R):
        rows_wide[k * c : (k + 1) * c, :] = buf_c[k].astype(F32)
    rows_v[...] = rows_wide[...].astype(BF16)
    load_orb.wait()

    chunk = 512 if nu % 512 == 0 else 256
    edge = (g == 0) | (g == G - 1)
    across = G - 1 - g
    falling = (g == 0) | ((2 * g >= G) & (g != G - 1))

    def store_new(mu):
        return pltpu.make_async_copy(new_v.at[mu], new_hbm.at[mu], new_sem.at[mu])

    @pl.loop(0, mu_dev)
    def _(mu):
        for copy in load(mu):
            copy.wait()
        eye = jnp.where(
            lax.broadcasted_iota(jnp.int32, shape, 0) == lax.broadcasted_iota(jnp.int32, shape, 1), 1.0, 0.0
        ).astype(BF16)

        @pl.loop(0, nu // chunk)
        def _(i):
            at = pl.ds(pl.multiple_of(i * chunk, chunk), chunk)
            correction = lax.dot_general(
                prev_v[mu, at, :], rows_v[...], (((1,), (1,)), ((), ())), preferred_element_type=F32
            )
            residual = (new_v[mu, at, :].astype(F32) - correction).astype(BF16)
            made = jnp.dot(residual, upper_v[...], preferred_element_type=F32).astype(BF16)
            new_v[mu, at, :] = made
            turned[:, at] = lax.dot_general(
                eye, made, (((1,), (1,)), ((), ())), preferred_element_type=F32
            ).astype(BF16)

        store_new(mu).start()
        slot = (g * R + r) * mu_dev + mu

        @pl.loop(0, G)
        def _(d):
            to = jnp.where(falling, G - 1 - d, d)
            cols = pl.ds(pl.multiple_of(to * j_dev, j_dev), j_dev)
            block_v[...] = jnp.dot(turned[...], orb_v[:, cols], preferred_element_type=F32)

            def deliver():
                for k in range(R):
                    peer = lax.rem(r + k, R)
                    src = send.at[mu, to, peer]
                    dst = out_hbm.at[slot]

                    def away():
                        remote(src, dst, send_sem, recv_sem, peer, to).start()

                    if k:
                        away()
                    else:
                        pl.when(to != g)(away)

                        @pl.when(to == g)
                        def _():
                            pltpu.make_async_copy(src, dst, own_sem).start()

            def keep():
                for k in range(R):
                    send[mu, to, k] = block_v[k * pl_dev : (k + 1) * pl_dev, :].astype(BF16)

            if not relayed(G):
                keep()
                deliver()
                return
            adds = ((g == 1) & (to == G - 1)) | ((g == G - 2) & (to == 0))
            hands = edge & (to == across)

            @pl.when(adds)
            def _():
                pltpu.make_async_copy(relay.at[mu], relay.at[mu], relay_sem.at[mu]).wait()
                for k in range(R):
                    mine = block_v[k * pl_dev : (k + 1) * pl_dev, :]
                    send[mu, to, k] = (mine + relay[mu, k].astype(F32)).astype(BF16)

            pl.when(jnp.logical_not(adds))(keep)

            @pl.when(hands)
            def _():
                via = jnp.where(g == 0, 1, G - 2)
                remote(send.at[mu, to], relay.at[mu], send_sem, relay_sem.at[mu], r, via).start()

            pl.when(jnp.logical_not(hands))(deliver)

    own = out_hbm.at[pl.ds(0, mu_dev)]
    pltpu.make_async_copy(own, own, own_sem).wait()
    for mu in range(mu_dev):
        store_new(mu).wait()
    every = out_hbm.at[pl.ds(0, (N - 1) * mu_dev)]
    pltpu.make_async_copy(every, every, send_sem).wait()
    if relayed(G):
        @pl.when(edge)
        def _():
            fewer = out_hbm.at[pl.ds(0, (N - R - 1) * mu_dev)]
            pltpu.make_async_copy(fewer, fewer, recv_sem).wait()

        @pl.when(jnp.logical_not(edge))
        def _():
            pltpu.make_async_copy(every, every, recv_sem).wait()
    else:
        pltpu.make_async_copy(every, every, recv_sem).wait()


def fused(picked, columns, previous, inverse, orbitals, R, G):
    mu_dev, nu, p = columns.shape
    k = previous.shape[2]
    c = p // R
    nj = orbitals.shape[1]
    hbm = pl.BlockSpec(memory_space=pl.ANY)
    vmem = pl.BlockSpec(memory_space=pltpu.VMEM)
    dma = pltpu.SemaphoreType.DMA
    return pl.pallas_call(
        functools.partial(fused_kernel, R, G),
        out_shape=(
            jax.ShapeDtypeStruct((R * G * mu_dev, c, nj // G), BF16),
            jax.ShapeDtypeStruct(columns.shape, BF16),
        ),
        in_specs=[vmem, hbm, hbm, vmem, hbm],
        out_specs=(hbm, hbm),
        scratch_shapes=[
            pltpu.VMEM((R, c, k), BF16),
            pltpu.VMEM((G, c, k), BF16),
            pltpu.VMEM((R, c, k), BF16),
            pltpu.VMEM((p, k), F32),
            pltpu.VMEM((p, k), BF16),
            pltpu.VMEM((p, p), BF16),
            pltpu.VMEM((mu_dev, nu, p), BF16),
            pltpu.VMEM((mu_dev, nu, k), BF16),
            pltpu.VMEM((nu, nj), BF16),
            pltpu.VMEM((p, nu), BF16),
            pltpu.VMEM((p, nj // G), F32),
            pltpu.VMEM((mu_dev, G, R, c, nj // G), BF16),
            pltpu.VMEM((mu_dev, R, c, nj // G), BF16),
            dma((R,)), dma((R,)), dma((G,)), dma((G,)), dma((R,)), dma((R,)),
            dma((2 * mu_dev + 1,)), dma((mu_dev,)), dma(()), dma(()), dma(()), dma((mu_dev,)),
        ],
        compiler_params=pltpu.CompilerParams(
            collective_id=0, has_side_effects=True, vmem_limit_bytes=60 * 1024 * 1024
        ),
        name="fused_exchange",
    )(picked, columns, previous, inverse, orbitals)


def block_kernel(part_ref, slab_ref, out_ref, half_ref, sorted_ref, slab_t_ref):
    groups, rows, _ = part_ref.shape
    mus = slab_ref.shape[0]
    block = out_ref.shape[0]
    vecs = rows // mus
    step = pl.program_id(0)
    g = lax.axis_index("grp")

    @pl.when(step == 0)
    def _():
        slab_t_ref[...] = slab_ref[...].astype(F32).T.astype(BF16)
        piece = 128

        @pl.loop(0, rows // piece)
        def _(i):
            at = pl.ds(pl.multiple_of(i * piece, piece), piece)
            total = jnp.zeros((piece, part_ref.shape[2]), F32)
            for k in range(groups):
                part = part_ref[k, at, :].astype(F32)
                if relayed(groups) and k in (0, groups - 1):
                    part = jnp.where(g == groups - 1 - k, 0.0, part)
                total = total + part
            half_ref[at, :] = total.astype(BF16)

        shift = mus.bit_length() - 1

        @pl.loop(0, rows // piece)
        def _(i):
            at = pl.ds(pl.multiple_of(i * piece, piece), piece)
            row = lax.broadcasted_iota(jnp.int32, (piece, rows), 0) + i * piece
            col = lax.broadcasted_iota(jnp.int32, (piece, rows), 1)
            source = (row & (mus - 1)) * vecs + lax.shift_right_logical(row, shift)
            pick = jnp.where(source == col, 1.0, 0.0).astype(BF16)
            sorted_ref[at, :] = jnp.dot(pick, half_ref[...], preferred_element_type=F32).astype(BF16)

    for q in range(block):
        at = pl.ds(pl.multiple_of((step * block + q) * mus, mus), mus)
        out_ref[q] = jnp.dot(slab_t_ref[...], sorted_ref[at, :], preferred_element_type=F32).astype(BF16)


def orbital_block(parts, slab):
    groups, rows, j = parts.shape
    mus, i = slab.shape
    assert mus & (mus - 1) == 0
    vecs = rows // mus
    block = 4 if vecs % 4 == 0 else 1
    return pl.pallas_call(
        block_kernel,
        grid=(vecs // block,),
        out_shape=jax.ShapeDtypeStruct((vecs, i, j), BF16),
        in_specs=[
            pl.BlockSpec((groups, rows, j), lambda s: (0, 0, 0)),
            pl.BlockSpec((mus, i), lambda s: (0, 0)),
        ],
        out_specs=pl.BlockSpec((block, i, j), lambda s: (s, 0, 0)),
        scratch_shapes=[
            pltpu.VMEM((rows, j), BF16),
            pltpu.VMEM((rows, j), BF16),
            pltpu.VMEM((i, mus), BF16),
        ],
        name="orbital_block",
    )(parts, slab)


def per_device(R, G, pivot_columns, previous, pivots, pivot_inverse, orbitals, slab_orbitals):
    mu_dev, nu_dev, prev_count = previous.shape
    count = pivot_columns.shape[2]
    nbas = nu_dev * G
    row_index = lax.axis_index("rows")
    grp_index = lax.axis_index("grp")
    first_local = pivots // nbas - row_index * mu_dev
    second_local = pivots % nbas - grp_index * nu_dev
    owned = (
        (first_local >= 0) & (first_local < mu_dev) & (second_local >= 0) & (second_local < nu_dev)
    )
    local_row = jnp.where(owned, first_local * nu_dev + second_local, 0)
    flat_prev = previous.reshape(mu_dev * nu_dev, prev_count)
    picked = jnp.where(
        owned[:, None], flat_prev.at[local_row].get(mode="promise_in_bounds"), jnp.zeros((), BF16)
    )
    parts, new_vectors = fused(
        picked.reshape(R, count // R, prev_count), pivot_columns, previous, pivot_inverse, orbitals, R, G
    )
    parts = parts.reshape(G, R * mu_dev * (count // R), orbitals.shape[1] // G)
    return new_vectors, orbital_block(parts, slab_orbitals)


def solution(mesh):
    R, G = mesh.shape["rows"], mesh.shape["grp"]
    in_specs = (P("rows", "grp", None), P("rows", "grp", None), P(), P(), P("grp", None), P())
    out_specs = (P("rows", "grp", None), P("rows", None, "grp"))
    return jax.shard_map(
        functools.partial(per_device, R, G), mesh=mesh, in_specs=in_specs, out_specs=out_specs,
        check_vma=False,
    )
```
